256 devices in a mesh: ens: 4 (over y), fsdp: 16 (over z, core), model: 4 (over x).
Axes of the slice: x: 4, y: 4, z: 8, core: 2. Of those that a mesh axis runs over, the one named last changes fastest.
Arguments:
- weight_gate: bfloat16 [8192, 8192], P(('ens', 'fsdp'), 'model'), parts along dimension 0, may hold values from -0.125 to 0.125
- low_gate: bfloat16 [8192, 32], P(('ens', 'fsdp')), parts along dimension 0, may hold values from -0.125 to 0.125
- high_gate: bfloat16 [128, 8192], P('ens', 'model'), parts along dimension 0, may hold values from -1 to 1
- weight_up: bfloat16 [8192, 8192], P(('ens', 'fsdp'), 'model'), parts along dimension 0, may hold values from -0.125 to 0.125
- low_up: bfloat16 [8192, 32], P(('ens', 'fsdp')), parts along dimension 0, may hold values from -0.125 to 0.125
- high_up: bfloat16 [128, 8192], P('ens', 'model'), parts along dimension 0, may hold values from -1 to 1
- norm_train: float32 [8192], P(('ens', 'fsdp', 'model')), parts along dimension 0, may hold values from 0.25 to 1.75
- norm_step: float32 [8192], P(('ens', 'fsdp', 'model')), parts along dimension 0, may hold values from -0.3 to 0.3
Outputs:
- final_gate: bfloat16 [32768, 2048], P(('ens', 'model')), parts along dimension 0
- final_up: bfloat16 [32768, 2048], P(('ens', 'model')), parts along dimension 0
- serve_norm: bfloat16 [8192], P('ens'), parts along dimension 0
The draws below stay inside these ranges and needn't reach their ends.
There are 4 independent parts, one for each index of `ens`. The reference program is written for one: setup_inputs(seed, part) draws one part's arguments, and reference() takes and returns one part's arrays. A program takes and returns all parts, laid end to end along the dimension named above; each array names one. Nothing has to cross between parts.
All inputs are finite; a program needn't handle non-finite values.
Results may differ from the reference program's by a relative error of at most 0.001.
Values may be sent and summed in bfloat16 or wider, within the bound.
No kernel may reach another device: no remote copies, remote signals or barrier semaphores. Data moves between devices by JAX's collectives and lax.ppermute only.
A program may use at most 128 MiB of HBM per device.

```python
import jax
import jax.numpy as jnp

D_MODEL = 2048
D_INNER = 8192
RANK = 32


def steps_of(own_key, shape, cuts, least, high):
    def one(dim, blocks):
        steps = jax.random.uniform(jax.random.fold_in(jax.random.fold_in(own_key, 6), dim), (blocks,), jnp.float32, least / len(cuts), high / len(cuts))
        return jnp.repeat(jnp.exp(steps), shape[dim] // blocks).reshape((-1,) + (1,) * (len(shape) - dim - 1))

    gain = one(*cuts[0])
    for cut in cuts[1:]:
        gain = gain * one(*cut)
    return gain


def bell_draw(own_key, shape, spread, limit, shards=(), held_as=jnp.bfloat16):
    loudness = steps_of(own_key, shape, shards, -0.22, 0.18) if shards else 1.0
    values = jax.random.normal(own_key, shape, jnp.float32) * spread * loudness
    return jnp.minimum(jnp.maximum(values, -limit), limit).astype(held_as)


def setup_inputs(seed: int = 0, part: int = 0) -> dict:
    keys = jax.random.split(jax.random.key(seed), 9)
    part_keys = jax.random.split(jax.random.fold_in(keys[8], part), 9)
    weight_gate = bell_draw(part_keys[0], (D_MODEL, D_INNER), D_MODEL ** -0.5, 0.125, ((0, 16), (1, 4)))
    low_gate = bell_draw(part_keys[1], (D_MODEL, RANK), D_MODEL ** -0.5, 0.125, ((0, 16),))
    high_gate = bell_draw(part_keys[2], (RANK, D_INNER), RANK ** -0.5, 1.0, ((1, 4),))
    weight_up = bell_draw(part_keys[3], (D_MODEL, D_INNER), D_MODEL ** -0.5, 0.125, ((0, 16), (1, 4)))
    low_up = bell_draw(part_keys[4], (D_MODEL, RANK), D_MODEL ** -0.5, 0.125, ((0, 16),))
    high_up = bell_draw(part_keys[5], (RANK, D_INNER), RANK ** -0.5, 1.0, ((1, 4),))
    norm_train = jnp.clip(1.0 + 0.15 * jax.random.normal(part_keys[6], (D_MODEL,), jnp.float32), 0.25, 1.75)
    norm_step = jnp.clip(jax.random.uniform(part_keys[7], (D_MODEL,), jnp.float32, -0.3, 0.3) * steps_of(part_keys[7], (D_MODEL,), ((0, 64),), -0.4, 0.0), -0.3, 0.3)
    return {"weight_gate": weight_gate, "low_gate": low_gate, "high_gate": high_gate, "weight_up": weight_up, "low_up": low_up, "high_up": high_up, "norm_train": norm_train, "norm_step": norm_step}


mix_rate = 2.0


def reference(weight_gate, low_gate, high_gate, weight_up, low_up, high_up, norm_train, norm_step):
    result_gate = weight_gate.astype(jnp.float32) + mix_rate * jnp.dot(low_gate, high_gate, preferred_element_type=jnp.float32)
    result_up = weight_up.astype(jnp.float32) + mix_rate * jnp.dot(low_up, high_up, preferred_element_type=jnp.float32)
    final_gate = result_gate.T.astype(jnp.bfloat16)
    final_up = result_up.T.astype(jnp.bfloat16)
    serve_norm = (norm_train + norm_step).astype(jnp.bfloat16)
    return final_gate, final_up, serve_norm
```

```python
import functools
import jax
import jax.numpy as jnp
from jax import lax
from jax.experimental import pallas as pl
from jax.experimental.pallas import tpu as pltpu
from jax.sharding import PartitionSpec as P


mix_rate = 2.0
RING = "fsdp"
MERGE_GRANT = 56 << 20
ANY = pl.BlockSpec(memory_space=pl.ANY)
VMEM = pl.BlockSpec(memory_space=pltpu.VMEM)


def paired(x, axis, bit):
    n = lax.axis_size(axis)
    return lax.ppermute(x, axis, [(i, i ^ bit) for i in range(n)])


def shifted(x, chips):
    n = lax.axis_size(RING)
    return lax.ppermute(x, RING, [(i, (i + 2 * chips) % n) for i in range(n)])


def swapped(x):
    n = lax.axis_size(RING)
    return lax.ppermute(x, RING, [(i, i ^ 1) for i in range(n)])


def merge_kernel(wg, lg, hg, wu, lu, hu, og, ou, wbuf, lbuf, hbuf, tbuf, isem, osem):
    mats = ((wg, lg, hg, og), (wu, lu, hu, ou))
    loads = [
        [
            pltpu.make_async_copy(src, buf.at[k], isem.at[k, i])
            for i, (src, buf) in enumerate(zip(mat[:3], (wbuf, lbuf, hbuf)))
        ]
        for k, mat in enumerate(mats)
    ]
    stores = [pltpu.make_async_copy(tbuf.at[k], mat[3], osem.at[k]) for k, mat in enumerate(mats)]
    for group in loads:
        for cp in group:
            cp.start()
    for k in range(2):
        for cp in loads[k]:
            cp.wait()
        add = lax.dot_general(
            lbuf[k], hbuf[k], (((0,), (0,)), ((), ())), preferred_element_type=jnp.float32
        )
        total = wbuf[k].astype(jnp.float32) + mix_rate * add
        tbuf[k] = total.astype(jnp.bfloat16).T
        stores[k].start()
    for cp in stores:
        cp.wait()


def merged(wg, lg, hg, wu, lu, hu):
    rows, cols = wg.shape
    rank = lg.shape[1]
    out = jax.ShapeDtypeStruct((cols, rows), jnp.bfloat16)
    return pl.pallas_call(
        merge_kernel,
        out_shape=(out, out),
        in_specs=[ANY] * 6,
        out_specs=(ANY, ANY),
        scratch_shapes=[
            pltpu.VMEM((2, rows, cols), jnp.bfloat16),
            pltpu.VMEM((2, rank, rows), jnp.bfloat16),
            pltpu.VMEM((2, rank, cols), jnp.bfloat16),
            pltpu.VMEM((2, cols, rows), jnp.bfloat16),
            pltpu.SemaphoreType.DMA((2, 3)),
            pltpu.SemaphoreType.DMA((2,)),
        ],
        compiler_params=pltpu.CompilerParams(vmem_limit_bytes=MERGE_GRANT),
        name="merge",
        cost_estimate=pl.CostEstimate(
            flops=4 * rows * cols * rank, bytes_accessed=8 * rows * cols, transcendentals=0
        ),
    )(wg, lg.T, hg, wu, lu.T, hu)


def place_kernel(units, aliased, *refs):
    n = len(units)
    outs = refs[n + 2 * aliased:n + 2 * aliased + 2]
    sem = refs[n + 2 * aliased + 2]
    me = lax.axis_index(RING)
    chips = lax.axis_size(RING) // 2
    copies = []
    for k, (which, hop, swap) in enumerate(units):
        block = refs[k]
        _, rows = block.shape
        core = lax.rem(me, 2)
        chip = lax.rem(lax.div(me, 2) + chips - hop, chips)
        owner = chip * 2 + (1 - core if swap else core)
        copies.append(pltpu.make_async_copy(
            block,
            outs[which].at[:, pl.ds(pl.multiple_of(owner * rows, rows), rows)],
            sem.at[k],
        ))
    for cp in copies:
        cp.start()
    for cp in copies:
        cp.wait()


def place(outs, shape, blocks, units):
    n = len(blocks)
    aliased = outs is not None
    operands = (*blocks, *outs) if aliased else tuple(blocks)
    out = jax.ShapeDtypeStruct(shape, jnp.bfloat16)
    return pl.pallas_call(
        functools.partial(place_kernel, units, int(aliased)),
        out_shape=(out, out),
        in_specs=[ANY] * len(operands),
        out_specs=(ANY, ANY),
        scratch_shapes=[pltpu.SemaphoreType.DMA((n,))],
        input_output_aliases={n: 0, n + 1: 1} if aliased else {},
        compiler_params=pltpu.CompilerParams(vmem_limit_bytes=1 << 20),
        name="place",
        cost_estimate=pl.CostEstimate(
            flops=1_000_000 * n, bytes_accessed=4 * n * blocks[0].size, transcendentals=0
        ),
    )(*operands)


def body(weight_gate, low_gate, high_gate, weight_up, low_up, high_up, norm_train, norm_step):
    rows, cols = weight_gate.shape
    chips = lax.axis_size(RING) // 2
    shape = (cols, rows * 2 * chips)
    far = chips // 2

    held = {}
    held["g", 0], held["u", 0] = merged(
        weight_gate, low_gate, high_gate, weight_up, low_up, high_up
    )
    for h in range(1, far + 1):
        held["g", h] = shifted(held["g", h - 1], 1)
        held["u", -h] = shifted(held["u", 1 - h], -1)
        if h < far:
            held["u", h] = shifted(held["u", h - 1], 1)
            held["g", -h] = shifted(held["g", 1 - h], -1)
    other = {k: swapped(v) for k, v in held.items()}

    def put(outs, keys, which=(False, True)):
        units = [("gu".index(w), h, s) for w, h in keys for s in which]
        blocks = [(other if s else held)[k] for k in keys for s in which]
        return place(outs, shape, blocks, units)

    outs = put(None, [("g", 0), ("u", 0)])
    for h in range(1, far):
        outs = put(outs, [("g", h), ("u", -h)])
        outs = put(outs, [("u", h), ("g", -h)])
    last = [("g", far), ("u", -far)]
    outs = put(outs, last, (False,))
    outs = put(outs, last, (True,))
    own = (norm_train + norm_step).astype(jnp.bfloat16)
    models = lax.axis_size("model")
    tile = (2 * chips, models * own.size)
    row = lax.broadcasted_iota(jnp.int32, tile, 0) == lax.axis_index(RING)
    lane = lax.broadcasted_iota(jnp.int32, tile, 1) // own.size == lax.axis_index("model")
    norm = jnp.where(row & lane, jnp.tile(own, models)[None], jnp.bfloat16(0))
    for axis, bit in NORM_STEPS:
        norm = norm + paired(norm, axis, bit)
    serve_norm = norm.reshape(-1)
    return outs[0], outs[1], serve_norm


NORM_STEPS = (
    (RING, 2), (RING, 4), ("model", 1),
    (RING, 8), ("model", 2), (RING, 1),
)


def solution(mesh):
    return jax.shard_map(
        body,
        mesh=mesh,
        in_specs=(
            P(("ens", "fsdp"), "model"),
            P(("ens", "fsdp"), None),
            P("ens", "model"),
            P(("ens", "fsdp"), "model"),
            P(("ens", "fsdp"), None),
            P("ens", "model"),
            P(("ens", "fsdp", "model")),
            P(("ens", "fsdp", "model")),
        ),
        out_specs=(P(("ens", "model"), None), P(("ens", "model"), None), P("ens")),
        check_vma=False,
    )
```

```python
import functools
import jax
import jax.numpy as jnp
from jax import lax
from jax.experimental import pallas as pl
from jax.experimental.pallas import tpu as pltpu
from jax.sharding import PartitionSpec as P


mix_rate = 2.0
RING = "fsdp"
LARGE, SMALL = 56 << 20, 8 << 20
ANY = pl.BlockSpec(memory_space=pl.ANY)
VMEM = pl.BlockSpec(memory_space=pltpu.VMEM)


def paired(x, axis, bit):
    n = lax.axis_size(axis)
    return lax.ppermute(x, axis, [(i, i ^ bit) for i in range(n)])


def shifted(x, chips):
    n = lax.axis_size(RING)
    return lax.ppermute(x, RING, [(i, (i + 2 * chips) % n) for i in range(n)])


def swapped(x):
    n = lax.axis_size(RING)
    return lax.ppermute(x, RING, [(i, i ^ 1) for i in range(n)])


def merge_kernel(place_own, wg, lg, hg, wu, lu, hu, og, ou, *refs):
    finals = refs[:2] if place_own else ()
    wbuf, lbuf, hbuf, tbuf, isem, osem = refs[len(finals):]
    mats = ((wg, lg, hg, og), (wu, lu, hu, ou))
    rows = wg.shape[0]
    rank = hg.shape[0]
    loads = [
        [
            pltpu.make_async_copy(src, buf.at[k], isem.at[k, i])
            for i, (src, buf) in enumerate(zip(
                (mat[0], mat[1].at[pl.ds(k * rank, rank), :], mat[2]), (wbuf, lbuf, hbuf)
            ))
        ]
        for k, mat in enumerate(mats)
    ]
    stores = [[pltpu.make_async_copy(tbuf.at[k], mat[3], osem.at[k, 0])] for k, mat in enumerate(mats)]
    for k, final in enumerate(finals):
        mine = pl.multiple_of(lax.axis_index(RING) * rows, rows)
        stores[k].append(
            pltpu.make_async_copy(tbuf.at[k], final.at[:, pl.ds(mine, rows)], osem.at[k, 1])
        )
    for group in loads:
        for cp in group:
            cp.start()
    for k in range(2):
        for cp in loads[k]:
            cp.wait()
        add = lax.dot_general(
            lbuf[k], hbuf[k], (((0,), (0,)), ((), ())), preferred_element_type=jnp.float32
        )
        total = wbuf[k].astype(jnp.float32) + mix_rate * add
        tbuf[k] = total.astype(jnp.bfloat16).T
        for cp in stores[k]:
            cp.start()
    for group in stores:
        for cp in group:
            cp.wait()


def merged(wg, lg, hg, wu, lu, hu, grant, final=None):
    rows, cols = wg.shape
    rank = hg.shape[0]
    out = jax.ShapeDtypeStruct((cols, rows), jnp.bfloat16)
    outs = (out, out)
    if final:
        outs += (jax.ShapeDtypeStruct(final, jnp.bfloat16),) * 2
    return pl.pallas_call(
        functools.partial(merge_kernel, bool(final)),
        out_shape=outs,
        in_specs=[ANY] * 6,
        out_specs=(ANY,) * len(outs),
        scratch_shapes=[
            pltpu.VMEM((2, rows, cols), jnp.bfloat16),
            pltpu.VMEM((2, rank, rows), jnp.bfloat16),
            pltpu.VMEM((2, rank, cols), jnp.bfloat16),
            pltpu.VMEM((2, cols, rows), jnp.bfloat16),
            pltpu.SemaphoreType.DMA((2, 3)),
            pltpu.SemaphoreType.DMA((2, 2)),
        ],
        compiler_params=pltpu.CompilerParams(vmem_limit_bytes=grant),
        name="mix",
        cost_estimate=pl.CostEstimate(flops=4 * rows * cols * rank, bytes_accessed=8 * rows * cols, transcendentals=0),
    )(wg, lg, hg, wu, lu, hu)


def place_kernel(units, *refs):
    n = len(units)
    outs = refs[n + 2:n + 4]
    sem = refs[n + 4]
    me = lax.axis_index(RING)
    chips = lax.axis_size(RING) // 2
    copies = []
    for k, (which, hop, swap, first) in enumerate(units):
        block = refs[k]
        size, rows = block.shape
        core = lax.rem(me, 2)
        chip = lax.rem(lax.div(me, 2) + chips - hop, chips)
        owner = chip * 2 + (1 - core if swap else core)
        copies.append(pltpu.make_async_copy(
            block,
            outs[which].at[pl.ds(first, size), pl.ds(pl.multiple_of(owner * rows, rows), rows)],
            sem.at[k],
        ))
    for cp in copies:
        cp.start()
    for cp in copies:
        cp.wait()


def place(outs, shape, blocks, units):
    n = len(blocks)
    operands = (*blocks, *outs)
    out = jax.ShapeDtypeStruct(shape, jnp.bfloat16)
    return pl.pallas_call(
        functools.partial(place_kernel, units),
        out_shape=(out, out),
        in_specs=[ANY] * len(operands),
        out_specs=(ANY, ANY),
        scratch_shapes=[pltpu.SemaphoreType.DMA((n,))],
        input_output_aliases={n: 0, n + 1: 1},
        compiler_params=pltpu.CompilerParams(vmem_limit_bytes=1 << 20),
        name="place",
        cost_estimate=pl.CostEstimate(
            flops=1_000_000 * n, bytes_accessed=4 * sum(b.size for b in blocks), transcendentals=0
        ),
    )(*operands)


def body(weight_gate, low_gate, high_gate, weight_up, low_up, high_up, norm_train, norm_step):
    rows, cols = weight_gate.shape
    chips = lax.axis_size(RING) // 2
    shape = (cols, rows * 2 * chips)
    far = chips // 2

    gate_above, up_below = shifted(weight_gate, 1), shifted(weight_up, -1)
    low = jnp.concatenate([low_gate.T, low_up.T], axis=0)
    low_above, low_below = shifted(low, 1), shifted(low, -1)
    up_above, gate_below = shifted(weight_up, 1), shifted(weight_gate, -1)

    def mix(gate, gate_low, up, up_low, grant, final=None):
        return merged(gate, gate_low, high_gate, up, up_low, high_up, grant, final)

    held = {}
    held["g", 0], held["u", 0], *outs = mix(weight_gate, low, weight_up, low, LARGE, shape)
    held["g", 1], held["u", -1] = mix(gate_above, low_above, up_below, low_below, SMALL)
    held["g", -1], held["u", 1] = mix(gate_below, low_below, up_above, low_above, SMALL)
    for h in range(2, far):
        held["g", h] = shifted(held["g", h - 1], 1)
        held["u", -h] = shifted(held["u", 1 - h], -1)
        held["u", h] = shifted(held["u", h - 1], 1)
        held["g", -h] = shifted(held["g", 1 - h], -1)
    held = {(*k, 0): v for k, v in held.items()}
    cut = cols - cols // 4
    for first, end in ((0, cut), (cut, cols)):
        held["g", far, first] = shifted(held["g", far - 1, 0][first:end], 1)
        held["u", -far, first] = shifted(held["u", 1 - far, 0][first:end], -1)

    other = {k: swapped(v) for k, v in held.items()}

    def put(outs, keys):
        units = [("gu".index(w), h, s, first) for w, h, first, s in keys]
        blocks = [(other if s else held)[w, h, first] for w, h, first, s in keys]
        return place(outs, shape, blocks, units)

    def both(*keys):
        return [(w, h, 0, s) for w, h in keys for s in (False, True)]

    for h in range(1, far):
        first = [("g", 0, 0, True), ("u", 0, 0, True)] if h == 1 else []
        outs = put(outs, first + both(("g", h), ("u", -h)))
        outs = put(outs, both(("u", h), ("g", -h)))
    last = [("g", far), ("u", -far)]
    outs = put(outs, [(*k, 0, False) for k in last])
    outs = put(outs, [(*k, 0, True) for k in last] + [(*k, cut, False) for k in last])
    outs = put(outs, [(*k, cut, True) for k in last])
    own = (norm_train + norm_step).astype(jnp.bfloat16)
    models = lax.axis_size("model")
    tile = (2 * chips, models * own.size)
    row = lax.broadcasted_iota(jnp.int32, tile, 0) == lax.axis_index(RING)
    lane = lax.broadcasted_iota(jnp.int32, tile, 1) // own.size == lax.axis_index("model")
    norm = jnp.where(row & lane, jnp.tile(own, models)[None], jnp.bfloat16(0))
    for axis, bit in NORM_STEPS:
        norm = norm + paired(norm, axis, bit)
    serve_norm = norm.reshape(-1)
    return outs[0], outs[1], serve_norm


NORM_STEPS = (
    (RING, 2), ("model", 1), (RING, 4),
    (RING, 8), ("model", 2), (RING, 1),
)


def solution(mesh):
    return jax.shard_map(
        body,
        mesh=mesh,
        in_specs=(
            P(("ens", "fsdp"), "model"),
            P(("ens", "fsdp"), None),
            P("ens", "model"),
            P(("ens", "fsdp"), "model"),
            P(("ens", "fsdp"), None),
            P("ens", "model"),
            P(("ens", "fsdp", "model")),
            P(("ens", "fsdp", "model")),
        ),
        out_specs=(P(("ens", "model"), None), P(("ens", "model"), None), P("ens")),
        check_vma=False,
    )
```

```python
import functools
import jax
import jax.numpy as jnp
from jax import lax
from jax.experimental import pallas as pl
from jax.experimental.pallas import tpu as pltpu
from jax.sharding import PartitionSpec as P


mix_rate = 2.0
RING = "fsdp"
LARGE, SMALL = 56 << 20, 8 << 20
LAST = (2048, 1536, 512)
ANY = pl.BlockSpec(memory_space=pl.ANY)
VMEM = pl.BlockSpec(memory_space=pltpu.VMEM)


def paired(x, axis, bit):
    n = lax.axis_size(axis)
    return lax.ppermute(x, axis, [(i, i ^ bit) for i in range(n)])


def onward(x):
    n = lax.axis_size(RING)
    return lax.ppermute(x, RING, [(i, (i + (2 if i % 2 == 0 else n - 2)) % n) for i in range(n)])


def swapped(x):
    n = lax.axis_size(RING)
    return lax.ppermute(x, RING, [(i, i ^ 1) for i in range(n)])


def merge_kernel(place_own, wg, wu, low, hg, hu, unit, *refs):
    finals = refs[:2] if place_own else ()
    wbuf, lbuf, hbuf, tbuf, lsem, isem, osem = refs[len(finals):]
    rows, cols = wg.shape
    rank = hg.shape[0]
    lows = pltpu.make_async_copy(low, lbuf, lsem)
    loads = [
        [
            pltpu.make_async_copy(src, buf.at[k], isem.at[k, i])
            for i, (src, buf) in enumerate(((w, wbuf), (h, hbuf)))
        ]
        for k, (w, h) in enumerate(((wg, hg), (wu, hu)))
    ]
    stores = [
        [pltpu.make_async_copy(tbuf.at[k], unit.at[pl.ds(k * cols, cols), :], osem.at[k, 0])]
        for k in range(2)
    ]
    for k, final in enumerate(finals):
        mine = pl.multiple_of(lax.axis_index(RING) * rows, rows)
        stores[k].append(
            pltpu.make_async_copy(tbuf.at[k], final.at[:, pl.ds(mine, rows)], osem.at[k, 1])
        )
    lows.start()
    for group in loads:
        for cp in group:
            cp.start()
    lows.wait()
    for k in range(2):
        for cp in loads[k]:
            cp.wait()
        add = lax.dot_general(
            lbuf[pl.ds(k * rank, rank), :], hbuf[k], (((0,), (0,)), ((), ())),
            preferred_element_type=jnp.float32,
        )
        total = wbuf[k].astype(jnp.float32) + mix_rate * add
        tbuf[k] = total.astype(jnp.bfloat16).T
        for cp in stores[k]:
            cp.start()
    for group in stores:
        for cp in group:
            cp.wait()


def merged(wg, wu, low, hg, hu, grant, final=None):
    rows, cols = wg.shape
    rank = hg.shape[0]
    outs = (jax.ShapeDtypeStruct((2 * cols, rows), jnp.bfloat16),)
    if final:
        outs += (jax.ShapeDtypeStruct(final, jnp.bfloat16),) * 2
    return pl.pallas_call(
        functools.partial(merge_kernel, bool(final)),
        out_shape=outs,
        in_specs=[ANY] * 5,
        out_specs=(ANY,) * len(outs),
        scratch_shapes=[
            pltpu.VMEM((2, rows, cols), jnp.bfloat16),
            pltpu.VMEM((2 * rank, rows), jnp.bfloat16),
            pltpu.VMEM((2, rank, cols), jnp.bfloat16),
            pltpu.VMEM((2, cols, rows), jnp.bfloat16),
            pltpu.SemaphoreType.DMA,
            pltpu.SemaphoreType.DMA((2, 2)),
            pltpu.SemaphoreType.DMA((2, 2)),
        ],
        compiler_params=pltpu.CompilerParams(vmem_limit_bytes=grant),
        name="mix",
        cost_estimate=pl.CostEstimate(
            flops=4 * rows * cols * rank, bytes_accessed=8 * rows * cols, transcendentals=0
        ),
    )(wg, wu, low, hg, hu)


def place_kernel(units, *refs):
    n = len(units)
    outs = refs[n + 2:n + 4]
    sem = refs[n + 4]
    me = lax.axis_index(RING)
    chips = lax.axis_size(RING) // 2
    z, core = lax.div(me, 2), lax.rem(me, 2)
    copies = []
    for k, (hops, kind, swap, first) in enumerate(units):
        size, rows = refs[k].shape
        cols = outs[0].shape[0]
        via = 1 - core if swap else core
        chip = lax.rem(z + chips - hops * (1 - 2 * via), chips)
        owner = chip * 2 + (1 - via if kind else via)
        for w in range(2):
            lo, hi = max(first, w * cols), min(first + size, (w + 1) * cols)
            if lo < hi:
                copies.append(pltpu.make_async_copy(
                    refs[k].at[pl.ds(lo - first, hi - lo), :],
                    outs[w].at[
                        pl.ds(lo - w * cols, hi - lo), pl.ds(pl.multiple_of(owner * rows, rows), rows)
                    ],
                    sem.at[k, w],
                ))
    for cp in copies:
        cp.start()
    for cp in copies:
        cp.wait()


def place(outs, blocks, units):
    n = len(blocks)
    operands = (*blocks, *outs)
    out = jax.ShapeDtypeStruct(outs[0].shape, jnp.bfloat16)
    return pl.pallas_call(
        functools.partial(place_kernel, units),
        out_shape=(out, out),
        in_specs=[ANY] * len(operands),
        out_specs=(ANY, ANY),
        scratch_shapes=[pltpu.SemaphoreType.DMA((n, 2))],
        input_output_aliases={n: 0, n + 1: 1},
        compiler_params=pltpu.CompilerParams(vmem_limit_bytes=1 << 20),
        name="place",
        cost_estimate=pl.CostEstimate(
            flops=1_000_000 * n, bytes_accessed=4 * sum(b.size for b in blocks), transcendentals=0
        ),
    )(*operands)


def body(weight_gate, low_gate, high_gate, weight_up, low_up, high_up, norm_train, norm_step):
    rows, cols = weight_gate.shape
    chips = lax.axis_size(RING) // 2
    shape = (cols, rows * 2 * chips)
    far = chips // 2

    raw_gate, raw_up = onward(weight_gate), onward(weight_up)
    low = jnp.concatenate([low_gate.T, low_up.T], axis=0)
    raw_low = onward(low)
    held, other = {}, {}
    held["A", 0], *outs = merged(weight_gate, weight_up, low, high_gate, high_up, LARGE, shape)
    other["A", 0] = swapped(held["A", 0])
    held["A", 1], = merged(raw_gate, raw_up, raw_low, high_gate, high_up, SMALL)
    held["B", 1] = onward(other["A", 0])
    for h in range(2, far):
        held["A", h] = onward(held["A", h - 1])
        held["B", h] = onward(held["B", h - 1])
    first_row, row = {}, 0
    for part, size in zip("abc", LAST):
        kind = f"A4{part}"
        held[kind, far] = onward(held["A", far - 1][row:row + size])
        first_row[kind], row = row, row + size
    for kind, h in held:
        if h:
            other[kind, h] = swapped(held[kind, h])

    def put(outs, keys):
        blocks = [(other if s else held)[kind, h] for kind, h, s in keys]
        units = [(h, int(kind == "B"), s, first_row.get(kind, 0)) for kind, h, s in keys]
        return place(outs, blocks, units)

    outs = put(outs, [("A", 0, True), ("A", 1, False), ("A", 1, True)])
    for h in range(1, far):
        if h > 1:
            outs = put(outs, [("A", h, False), ("A", h, True)])
        outs = put(outs, [("B", h, False), ("B", h, True)])
    outs = put(outs, [("A4a", far, False)])
    outs = put(outs, [("A4a", far, True), ("A4b", far, False)])
    outs = put(outs, [("A4b", far, True), ("A4c", far, False)])
    outs = put(outs, [("A4c", far, True)])
    own = (norm_train + norm_step).astype(jnp.bfloat16)
    models = lax.axis_size("model")
    tile = (2 * chips, models * own.size)
    row = lax.broadcasted_iota(jnp.int32, tile, 0) == lax.axis_index(RING)
    lane = lax.broadcasted_iota(jnp.int32, tile, 1) // own.size == lax.axis_index("model")
    norm = jnp.where(row & lane, jnp.tile(own, models)[None], jnp.bfloat16(0))
    for axis, bit in NORM_STEPS:
        norm = norm + paired(norm, axis, bit)
    serve_norm = norm.reshape(-1)
    return outs[0], outs[1], serve_norm


NORM_STEPS = (
    (RING, 2), ("model", 1), (RING, 4),
    (RING, 8), ("model", 2), (RING, 1),
)


def solution(mesh):
    return jax.shard_map(
        body,
        mesh=mesh,
        in_specs=(
            P(("ens", "fsdp"), "model"),
            P(("ens", "fsdp"), None),
            P("ens", "model"),
            P(("ens", "fsdp"), "model"),
            P(("ens", "fsdp"), None),
            P("ens", "model"),
            P(("ens", "fsdp", "model")),
            P(("ens", "fsdp", "model")),
        ),
        out_specs=(P(("ens", "model"), None), P(("ens", "model"), None), P("ens")),
        check_vma=False,
    )
```

```python
import functools
import jax
import jax.numpy as jnp
from jax import lax
from jax.experimental import pallas as pl
from jax.experimental.pallas import tpu as pltpu
from jax.sharding import PartitionSpec as P


mix_rate = 2.0
RING = "fsdp"
LARGE, SMALL = 56 << 20, 8 << 20
LAST = (2048, 1536, 512)
ANY = pl.BlockSpec(memory_space=pl.ANY)
VMEM = pl.BlockSpec(memory_space=pltpu.VMEM)


def paired(x, axis, bit):
    n = lax.axis_size(axis)
    return lax.ppermute(x, axis, [(i, i ^ bit) for i in range(n)])


def onward(x):
    n = lax.axis_size(RING)
    return lax.ppermute(x, RING, [(i, (i + (2 if i % 2 == 1 else n - 2)) % n) for i in range(n)])


def swapped(x):
    n = lax.axis_size(RING)
    return lax.ppermute(x, RING, [(i, i ^ 1) for i in range(n)])


def merge_kernel(place_own, wg, wu, low, hg, hu, unit, *refs):
    finals = refs[:2] if place_own else ()
    wbuf, lbuf, hbuf, tbuf, lsem, isem, osem = refs[len(finals):]
    rows, cols = wg.shape
    rank = hg.shape[0]
    lows = pltpu.make_async_copy(low, lbuf, lsem)
    loads = [
        [
            pltpu.make_async_copy(src, buf.at[k], isem.at[k, i])
            for i, (src, buf) in enumerate(((w, wbuf), (h, hbuf)))
        ]
        for k, (w, h) in enumerate(((wg, hg), (wu, hu)))
    ]
    stores = [
        [pltpu.make_async_copy(tbuf.at[k], unit.at[pl.ds(k * cols, cols), :], osem.at[k, 0])]
        for k in range(2)
    ]
    for k, final in enumerate(finals):
        mine = pl.multiple_of(lax.axis_index(RING) * rows, rows)
        stores[k].append(
            pltpu.make_async_copy(tbuf.at[k], final.at[:, pl.ds(mine, rows)], osem.at[k, 1])
        )
    lows.start()
    for group in loads:
        for cp in group:
            cp.start()
    lows.wait()
    for k in range(2):
        for cp in loads[k]:
            cp.wait()
        add = lax.dot_general(
            lbuf[pl.ds(k * rank, rank), :], hbuf[k], (((0,), (0,)), ((), ())),
            preferred_element_type=jnp.float32,
        )
        total = wbuf[k].astype(jnp.float32) + mix_rate * add
        tbuf[k] = total.astype(jnp.bfloat16).T
        for cp in stores[k]:
            cp.start()
    for group in stores:
        for cp in group:
            cp.wait()


def merged(wg, wu, low, hg, hu, grant, final=None):
    rows, cols = wg.shape
    rank = hg.shape[0]
    outs = (jax.ShapeDtypeStruct((2 * cols, rows), jnp.bfloat16),)
    if final:
        outs += (jax.ShapeDtypeStruct(final, jnp.bfloat16),) * 2
    return pl.pallas_call(
        functools.partial(merge_kernel, bool(final)),
        out_shape=outs,
        in_specs=[ANY] * 5,
        out_specs=(ANY,) * len(outs),
        scratch_shapes=[
            pltpu.VMEM((2, rows, cols), jnp.bfloat16),
            pltpu.VMEM((2 * rank, rows), jnp.bfloat16),
            pltpu.VMEM((2, rank, cols), jnp.bfloat16),
            pltpu.VMEM((2, cols, rows), jnp.bfloat16),
            pltpu.SemaphoreType.DMA,
            pltpu.SemaphoreType.DMA((2, 2)),
            pltpu.SemaphoreType.DMA((2, 2)),
        ],
        compiler_params=pltpu.CompilerParams(vmem_limit_bytes=grant),
        name="mix",
        cost_estimate=pl.CostEstimate(
            flops=4 * rows * cols * rank, bytes_accessed=8 * rows * cols, transcendentals=0
        ),
    )(wg, wu, low, hg, hu)


def place_kernel(units, *refs):
    n = len(units)
    outs = refs[n + 2:n + 4]
    sem = refs[n + 4]
    me = lax.axis_index(RING)
    chips = lax.axis_size(RING) // 2
    z, core = lax.div(me, 2), lax.rem(me, 2)
    copies = []
    for k, (hops, kind, swap, first) in enumerate(units):
        size, rows = refs[k].shape
        cols = outs[0].shape[0]
        via = 1 - core if swap else core
        chip = lax.rem(z + chips - hops * (2 * via - 1), chips)
        owner = chip * 2 + (1 - via if kind else via)
        for w in range(2):
            lo, hi = max(first, w * cols), min(first + size, (w + 1) * cols)
            if lo < hi:
                copies.append(pltpu.make_async_copy(
                    refs[k].at[pl.ds(lo - first, hi - lo), :],
                    outs[w].at[
                        pl.ds(lo - w * cols, hi - lo), pl.ds(pl.multiple_of(owner * rows, rows), rows)
                    ],
                    sem.at[k, w],
                ))
    for cp in copies:
        cp.start()
    for cp in copies:
        cp.wait()


def place(outs, blocks, units):
    n = len(blocks)
    operands = (*blocks, *outs)
    out = jax.ShapeDtypeStruct(outs[0].shape, jnp.bfloat16)
    return pl.pallas_call(
        functools.partial(place_kernel, units),
        out_shape=(out, out),
        in_specs=[VMEM] * n + [ANY] * 2,
        out_specs=(ANY, ANY),
        scratch_shapes=[pltpu.SemaphoreType.DMA((n, 2))],
        input_output_aliases={n: 0, n + 1: 1},
        compiler_params=pltpu.CompilerParams(
            vmem_limit_bytes=(1 << 20) + 2 * sum(b.size for b in blocks)
        ),
        name="place",
        cost_estimate=pl.CostEstimate(
            flops=1_000_000 * n, bytes_accessed=4 * sum(b.size for b in blocks), transcendentals=0
        ),
    )(*operands)


def body(weight_gate, low_gate, high_gate, weight_up, low_up, high_up, norm_train, norm_step):
    rows, cols = weight_gate.shape
    chips = lax.axis_size(RING) // 2
    shape = (cols, rows * 2 * chips)
    far = chips // 2

    raw_gate, raw_up = onward(weight_gate), onward(weight_up)
    low = jnp.concatenate([low_gate.T, low_up.T], axis=0)
    raw_low = onward(low)
    held, other = {}, {}
    held["A", 0], *outs = merged(weight_gate, weight_up, low, high_gate, high_up, LARGE, shape)
    other["A", 0] = swapped(held["A", 0])
    held["A", 1], = merged(raw_gate, raw_up, raw_low, high_gate, high_up, SMALL)
    held["B", 1] = onward(other["A", 0])
    for h in range(2, far):
        held["A", h] = onward(held["A", h - 1])
        held["B", h] = onward(held["B", h - 1])
    first_row, row = {}, 0
    for part, size in zip("abc", LAST):
        kind = f"A4{part}"
        held[kind, far] = onward(held["A", far - 1][row:row + size])
        first_row[kind], row = row, row + size
    for kind, h in held:
        if h:
            other[kind, h] = swapped(held[kind, h])

    def put(outs, keys):
        blocks = [(other if s else held)[kind, h] for kind, h, s in keys]
        units = [(h, int(kind == "B"), s, first_row.get(kind, 0)) for kind, h, s in keys]
        return place(outs, blocks, units)

    outs = put(outs, [("A", 0, True), ("A", 1, False), ("A", 1, True)])
    for h in range(1, far):
        if h > 1:
            outs = put(outs, [("A", h, False), ("A", h, True)])
        outs = put(outs, [("B", h, False), ("B", h, True)])
    outs = put(outs, [("A4a", far, False)])
    outs = put(outs, [("A4a", far, True), ("A4b", far, False)])
    outs = put(outs, [("A4b", far, True), ("A4c", far, False)])
    outs = put(outs, [("A4c", far, True)])
    own = (norm_train + norm_step).astype(jnp.bfloat16)
    models = lax.axis_size("model")
    tile = (2 * chips, models * own.size)
    row = lax.broadcasted_iota(jnp.int32, tile, 0) == lax.axis_index(RING)
    lane = lax.broadcasted_iota(jnp.int32, tile, 1) // own.size == lax.axis_index("model")
    norm = jnp.where(row & lane, jnp.tile(own, models)[None], jnp.bfloat16(0))
    for axis, bit in NORM_STEPS:
        norm = norm + paired(norm, axis, bit)
    serve_norm = norm.reshape(-1)
    return outs[0], outs[1], serve_norm


NORM_STEPS = (
    ("model", 1), ("model", 2), (RING, 2),
    (RING, 4), (RING, 8), (RING, 1),
)


def solution(mesh):
    return jax.shard_map(
        body,
        mesh=mesh,
        in_specs=(
            P(("ens", "fsdp"), "model"),
            P(("ens", "fsdp"), None),
            P("ens", "model"),
            P(("ens", "fsdp"), "model"),
            P(("ens", "fsdp"), None),
            P("ens", "model"),
            P(("ens", "fsdp", "model")),
            P(("ens", "fsdp", "model")),
        ),
        out_specs=(P(("ens", "model"), None), P(("ens", "model"), None), P("ens")),
        check_vma=False,
    )
```

```python
import functools
import jax
import jax.numpy as jnp
from jax import lax
from jax.experimental import pallas as pl
from jax.experimental.pallas import tpu as pltpu
from jax.sharding import PartitionSpec as P


mix_rate = 2.0
RING = "fsdp"
LARGE, SMALL = 56 << 20, 8 << 20
LAST = (2048, 1536, 512)
ANY = pl.BlockSpec(memory_space=pl.ANY)
VMEM = pl.BlockSpec(memory_space=pltpu.VMEM)


def paired(x, axis, bit):
    n = lax.axis_size(axis)
    return lax.ppermute(x, axis, [(i, i ^ bit) for i in range(n)])


def onward(x):
    n = lax.axis_size(RING)
    return lax.ppermute(x, RING, [(i, (i + (2 if i % 2 == 1 else n - 2)) % n) for i in range(n)])


def swapped(x):
    n = lax.axis_size(RING)
    return lax.ppermute(x, RING, [(i, i ^ 1) for i in range(n)])


def merge_kernel(parts, place_own, *refs):
    lows, (wg, wu, hg, hu, unit), refs = refs[:parts], refs[parts:parts + 5], refs[parts + 5:]
    finals = refs[:2] if place_own else ()
    wbuf, lbuf, hbuf, tbuf, lsem, isem, osem = refs[len(finals):]
    rows, cols = wg.shape
    rank = hg.shape[0]
    size = 2 * rank // parts
    lows = [
        pltpu.make_async_copy(low, lbuf.at[pl.ds(i * size, size), :], lsem.at[i])
        for i, low in enumerate(lows)
    ]
    loads = [
        [
            pltpu.make_async_copy(src, buf.at[k], isem.at[k, i])
            for i, (src, buf) in enumerate(((w, wbuf), (h, hbuf)))
        ]
        for k, (w, h) in enumerate(((wg, hg), (wu, hu)))
    ]
    stores = [
        [pltpu.make_async_copy(tbuf.at[k], unit.at[pl.ds(k * cols, cols), :], osem.at[k, 0])]
        for k in range(2)
    ]
    for k, final in enumerate(finals):
        mine = pl.multiple_of(lax.axis_index(RING) * rows, rows)
        stores[k].append(
            pltpu.make_async_copy(tbuf.at[k], final.at[:, pl.ds(mine, rows)], osem.at[k, 1])
        )
    for group in (lows, *loads):
        for cp in group:
            cp.start()
    for cp in lows:
        cp.wait()
    for k in range(2):
        for cp in loads[k]:
            cp.wait()
        add = lax.dot_general(
            lbuf[pl.ds(k * rank, rank), :], hbuf[k], (((0,), (0,)), ((), ())),
            preferred_element_type=jnp.float32,
        )
        total = wbuf[k].astype(jnp.float32) + mix_rate * add
        tbuf[k] = total.astype(jnp.bfloat16).T
        for cp in stores[k]:
            cp.start()
    for group in stores:
        for cp in group:
            cp.wait()


def merged(wg, wu, lows, hg, hu, grant, final=None):
    rows, cols = wg.shape
    rank = hg.shape[0]
    outs = (jax.ShapeDtypeStruct((2 * cols, rows), jnp.bfloat16),)
    if final:
        outs += (jax.ShapeDtypeStruct(final, jnp.bfloat16),) * 2
    return pl.pallas_call(
        functools.partial(merge_kernel, len(lows), bool(final)),
        out_shape=outs,
        in_specs=[ANY] * (4 + len(lows)),
        out_specs=(ANY,) * len(outs),
        scratch_shapes=[
            pltpu.VMEM((2, rows, cols), jnp.bfloat16),
            pltpu.VMEM((2 * rank, rows), jnp.bfloat16),
            pltpu.VMEM((2, rank, cols), jnp.bfloat16),
            pltpu.VMEM((2, cols, rows), jnp.bfloat16),
            pltpu.SemaphoreType.DMA((2,)),
            pltpu.SemaphoreType.DMA((2, 2)),
            pltpu.SemaphoreType.DMA((2, 2)),
        ],
        compiler_params=pltpu.CompilerParams(vmem_limit_bytes=grant),
        name="mix",
        cost_estimate=pl.CostEstimate(flops=4 * rows * cols * rank, bytes_accessed=8 * rows * cols, transcendentals=0),
    )(*lows, wg, wu, hg, hu)


def place_kernel(units, *refs):
    n = len(units)
    outs = refs[n + 2:n + 4]
    sem = refs[n + 4]
    me = lax.axis_index(RING)
    chips = lax.axis_size(RING) // 2
    z, core = lax.div(me, 2), lax.rem(me, 2)
    copies = []
    for k, (hops, kind, swap, first) in enumerate(units):
        size, rows = refs[k].shape
        cols = outs[0].shape[0]
        via = 1 - core if swap else core
        chip = lax.rem(z + chips - hops * (2 * via - 1), chips)
        owner = chip * 2 + (1 - via if kind else via)
        for w in range(2):
            lo, hi = max(first, w * cols), min(first + size, (w + 1) * cols)
            if lo < hi:
                copies.append(pltpu.make_async_copy(
                    refs[k].at[pl.ds(lo - first, hi - lo), :],
                    outs[w].at[
                        pl.ds(lo - w * cols, hi - lo), pl.ds(pl.multiple_of(owner * rows, rows), rows)
                    ],
                    sem.at[k, w],
                ))
    for cp in copies:
        cp.start()
    for cp in copies:
        cp.wait()


def place(outs, blocks, units):
    n = len(blocks)
    operands = (*blocks, *outs)
    out = jax.ShapeDtypeStruct(outs[0].shape, jnp.bfloat16)
    return pl.pallas_call(
        functools.partial(place_kernel, units),
        out_shape=(out, out),
        in_specs=[VMEM] * n + [ANY] * 2,
        out_specs=(ANY, ANY),
        scratch_shapes=[pltpu.SemaphoreType.DMA((n, 2))],
        input_output_aliases={n: 0, n + 1: 1},
        compiler_params=pltpu.CompilerParams(
            vmem_limit_bytes=(1 << 20) + 2 * sum(b.size for b in blocks)
        ),
        name="place",
        cost_estimate=pl.CostEstimate(
            flops=1_000_000 * n, bytes_accessed=4 * sum(b.size for b in blocks), transcendentals=0
        ),
    )(*operands)


def body(weight_gate, low_gate, high_gate, weight_up, low_up, high_up, norm_train, norm_step):
    rows, cols = weight_gate.shape
    chips = lax.axis_size(RING) // 2
    shape = (cols, rows * 2 * chips)
    far = chips // 2

    raw_gate, raw_up = onward(weight_gate), onward(weight_up)
    low = jnp.concatenate([low_gate.T, low_up.T], axis=0)
    raw_low = onward(low)
    held, other = {}, {}
    held["A", 0], *outs = merged(weight_gate, weight_up, (low_gate.T, low_up.T), high_gate, high_up, LARGE, shape)
    other["A", 0] = swapped(held["A", 0])
    held["A", 1], = merged(raw_gate, raw_up, (raw_low,), high_gate, high_up, SMALL)
    held["B", 1] = onward(other["A", 0])
    for h in range(2, far):
        held["A", h] = onward(held["A", h - 1])
        held["B", h] = onward(held["B", h - 1])
    first_row, row = {}, 0
    for part, size in zip("abc", LAST):
        kind = f"A4{part}"
        held[kind, far] = onward(held["A", far - 1][row:row + size])
        first_row[kind], row = row, row + size
    for kind, h in held:
        if h:
            other[kind, h] = swapped(held[kind, h])

    def put(outs, keys):
        blocks = [(other if s else held)[kind, h] for kind, h, s in keys]
        units = [(h, int(kind == "B"), s, first_row.get(kind, 0)) for kind, h, s in keys]
        return place(outs, blocks, units)

    outs = put(outs, [("A", 0, True), ("A", 1, False), ("A", 1, True)])
    for h in range(1, far):
        if h > 1:
            outs = put(outs, [("A", h, False), ("A", h, True)])
        outs = put(outs, [("B", h, False), ("B", h, True)])
    outs = put(outs, [("A4a", far, False)])
    outs = put(outs, [("A4a", far, True), ("A4b", far, False)])
    outs = put(outs, [("A4b", far, True), ("A4c", far, False)])
    outs = put(outs, [("A4c", far, True)])
    own = (norm_train + norm_step).astype(jnp.bfloat16)
    models = lax.axis_size("model")
    tile = (2 * chips, models * own.size)
    row = lax.broadcasted_iota(jnp.int32, tile, 0) == lax.axis_index(RING)
    lane = lax.broadcasted_iota(jnp.int32, tile, 1) // own.size == lax.axis_index("model")
    norm = jnp.where(row & lane, jnp.tile(own, models)[None], jnp.bfloat16(0))
    for axis, bit in NORM_STEPS:
        norm = norm + paired(norm, axis, bit)
    serve_norm = norm.reshape(-1)
    return outs[0], outs[1], serve_norm


NORM_STEPS = (
    ("model", 1), ("model", 2), (RING, 2),
    (RING, 4), (RING, 8), (RING, 1),
)


def solution(mesh):
    return jax.shard_map(
        body,
        mesh=mesh,
        in_specs=(
            P(("ens", "fsdp"), "model"),
            P(("ens", "fsdp"), None),
            P("ens", "model"),
            P(("ens", "fsdp"), "model"),
            P(("ens", "fsdp"), None),
            P("ens", "model"),
            P(("ens", "fsdp", "model")),
            P(("ens", "fsdp", "model")),
        ),
        out_specs=(P(("ens", "model"), None), P(("ens", "model"), None), P("ens")),
        check_vma=False,
    )
```
